32 devices in a mesh: ep: 4 (over x, core), fsdp: 8 (over z, y).
Axes of the slice: x: 2, y: 2, z: 4, core: 2. Of those that a mesh axis runs over, the one named last changes fastest.
Arguments:
- master_gate: float32 [128, 2048, 768], P('ep', 'fsdp'), may hold values from -0.1875 to 0.1875
- master_up: float32 [128, 2048, 768], P('ep', 'fsdp'), may hold values from -0.1875 to 0.1875
- router_weight: float32 [2048, 128], P('fsdp', 'ep'), may hold values from -0.125 to 0.125
- router_gain: float32 [2048], P('fsdp'), may hold values from 0.25 to 1.75
Outputs:
- final_gate: bfloat16 [128, 2048, 768], P(('ep', 'fsdp'))
- final_up: bfloat16 [128, 2048, 768], P(('ep', 'fsdp'))
- scale_gate: float32 [128, 768], P(('ep', 'fsdp'))
- scale_up: float32 [128, 768], P(('ep', 'fsdp'))
- serve_router: bfloat16 [2048, 128], replicated
The draws below stay inside these ranges and needn't reach their ends.
All inputs are finite; a program needn't handle non-finite values.
Results may differ from the reference program's by a relative error of at most 0.001.
Values may be sent and summed in bfloat16 or wider, within the bound.
A program may use at most 192 MiB of HBM per device.

```python
import jax
import jax.numpy as jnp
from jax import lax

EXPERTS = 128
D_MODEL = 2048
D_EXPERT = 768


def with_spikes(drawn, own_key, source, target, blocks, factor):
    owner, partner = [(jnp.arange(drawn.shape[axis_at]) // (drawn.shape[axis_at] // blocks)).reshape([-1 if axis == axis_at else 1 for axis in range(drawn.ndim)]) for axis_at in (source, target)]
    chosen = jax.random.permutation(own_key, blocks)[partner]
    strong = (owner == chosen) | (owner == (partner + blocks // 2) % blocks)
    return jnp.where(strong, factor * drawn, drawn)


def level_of(stream_key, dims, pieces, least, high):
    loudness = 1.0
    for dim, parts in pieces:
        heights = jax.random.uniform(jax.random.fold_in(jax.random.fold_in(stream_key, 6), dim), (parts,), jnp.float32, least / len(pieces), high / len(pieces))
        loudness = loudness * jnp.repeat(jnp.exp(heights), dims[dim] // parts).reshape((-1,) + (1,) * (len(dims) - 1 - dim))
    return loudness


def noise(rng, shape, scale, limit, pieces=(), kind=jnp.bfloat16):
    result = scale * jax.random.normal(rng, shape, jnp.float32)
    if pieces:
        result = result * level_of(rng, shape, pieces, -0.22, 0.18)
    return jnp.clip(result, -limit, limit).astype(kind)


def gaussian_with(stream_key, extent, spread, most, cuts, heavy, kind=jnp.bfloat16):
    result = spread * jax.random.normal(stream_key, extent, jnp.float32)
    if cuts:
        result = result * level_of(stream_key, extent, cuts, -0.22, 0.18)
    return jnp.clip(with_spikes(result, jax.random.fold_in(stream_key, 3), *heavy), -most, most).astype(kind)


def setup_inputs(seed: int = 0) -> dict:
    streams_of = jax.random.split(jax.random.key(seed), 5)
    return {
        "master_gate": gaussian_with(streams_of[0], (EXPERTS, D_MODEL, D_EXPERT), D_MODEL ** -0.5, 0.1875, ((0, 4), (1, 8)), (1, 2, 8, 2.0), jnp.float32),
        "master_up": gaussian_with(streams_of[1], (EXPERTS, D_MODEL, D_EXPERT), D_MODEL ** -0.5, 0.1875, ((0, 4), (1, 8)), (1, 2, 8, 2.0), jnp.float32),
        "router_weight": noise(streams_of[2], (D_MODEL, EXPERTS), D_MODEL ** -0.5, 0.125, ((0, 8), (1, 4)), jnp.float32),
        "router_gain": jnp.clip(1.0 + 0.15 * jax.random.normal(streams_of[3], (D_MODEL,), jnp.float32), 0.25, 1.75),
    }


def reference(master_gate, master_up, router_weight, router_gain):
    scale_gate = jnp.sqrt(lax.optimization_barrier(jnp.sum(master_gate * master_gate, axis=1)))
    final_gate = (master_gate / jnp.expand_dims(scale_gate, 1)).astype(jnp.bfloat16)
    scale_up = jnp.sqrt(lax.optimization_barrier(jnp.sum(master_up * master_up, axis=1)))
    final_up = (master_up / jnp.expand_dims(scale_up, 1)).astype(jnp.bfloat16)
    serve_router = (router_weight * router_gain[:, None]).astype(jnp.bfloat16)
    return (final_gate, final_up, scale_gate, scale_up, serve_router)
```

```python
import functools

import jax
import jax.numpy as jnp
from jax import lax
from jax.experimental import pallas as pl
from jax.experimental.pallas import tpu as pltpu
from jax.sharding import PartitionSpec as P

MESH = pl.DeviceIdType.MESH
RING = 3


def kernel(
    groups, members, local, rows,
    gate, up, part_router,
    final_gate, final_up, scale_gate, scale_up, router,
    held, narrow, partial, arrived, scales,
    load_sem, send_sem, recv_sem, own_sem,
    sum_send, sum_recv, scale_send, scale_recv,
    row_send, row_recv, col_send, col_recv, router_sem,
):
    group, me = lax.axis_index("ep"), lax.axis_index("fsdp")
    steps = 2 * local

    def peer(j):
        return lax.rem(me + j, members)

    def group_peer(j):
        return lax.rem(group + j, groups)

    def source(step):
        return (gate, up)[step // local], (final_gate, final_up)[step // local], step % local

    order = [*range(1, steps), *range(1, steps)]

    def load(step, slot, j):
        master, _, index = source(step)
        return pltpu.make_async_copy(
            master.at[peer(j) * local + index], held.at[slot, j], load_sem.at[slot, j]
        )

    def start_load(step, slot):
        @pl.loop(0, members)
        def _(j):
            load(step, slot, j).start()

    def start_place(place):
        if place < len(order):
            start_load(order[place], 1 + place % RING)

    def sum_copy(step, j):
        return pltpu.make_async_remote_copy(
            src_ref=partial.at[step, j], dst_ref=arrived.at[step, j],
            send_sem=sum_send.at[step, j], recv_sem=sum_recv.at[step, j],
            device_id=(group, peer(j)), device_id_type=MESH,
        )

    def scale_copy(step, j):
        return pltpu.make_async_remote_copy(
            src_ref=scales.at[step, 0], dst_ref=scales.at[step, j],
            send_sem=scale_send.at[step, j], recv_sem=scale_recv.at[step, j],
            device_id=(group, peer(j)), device_id_type=MESH,
        )

    def my_rows(final, index):
        return final.at[index, pl.ds(pl.multiple_of(me * rows, rows), rows), :]

    def data_copy(step, j):
        _, final, index = source(step)
        return pltpu.make_async_remote_copy(
            src_ref=narrow.at[step % RING, j], dst_ref=my_rows(final, index),
            send_sem=send_sem.at[step, j], recv_sem=recv_sem.at[step, j],
            device_id=(group, peer(j)), device_id_type=MESH,
        )

    def own_copy(step):
        _, final, index = source(step)
        return pltpu.make_async_copy(narrow.at[step % RING, 0], my_rows(final, index), own_sem.at[step])

    width, depth = part_router.shape
    my_group_rows = pl.ds(pl.multiple_of(group * width, width), width)
    my_block = router.at[my_group_rows, pl.ds(pl.multiple_of(me * depth, depth), depth)]

    def row_copy(j):
        return pltpu.make_async_remote_copy(
            src_ref=part_router, dst_ref=my_block, send_sem=row_send.at[j], recv_sem=row_recv.at[j],
            device_id=(group, peer(j)), device_id_type=MESH,
        )

    def col_copy(j):
        return pltpu.make_async_remote_copy(
            src_ref=router.at[my_group_rows, :], dst_ref=router.at[my_group_rows, :],
            send_sem=col_send.at[j], recv_sem=col_recv.at[j],
            device_id=(group_peer(j), me), device_id_type=MESH,
        )

    start_load(0, 0)
    for place in range(RING):
        start_place(place)

    barrier = pltpu.get_barrier_semaphore()
    for j in range(1, members):
        pl.semaphore_signal(barrier, inc=1, device_id=(group, peer(j)), device_id_type=MESH)
    for j in range(1, groups):
        pl.semaphore_signal(barrier, inc=1, device_id=(group_peer(j), me), device_id_type=MESH)
    pl.semaphore_wait(barrier, members + groups - 2)

    def sums(step, slot):
        @pl.loop(0, members)
        def _(j):
            load(step, slot, j).wait()
            block = held[slot, j]
            partial[step, j] = jnp.sum(block * block, axis=0, keepdims=True)

        @pl.loop(1, members)
        def _(j):
            sum_copy(step, j).start()

    def total(step):
        @pl.loop(1, members)
        def _(j):
            sum_copy(step, j).wait_recv()

        value = partial[step, 0]
        for j in range(1, members):
            value = value + arrived[step, j]
        value = jnp.sqrt(value)
        scales[step, 0] = value
        index = step % local
        (scale_gate, scale_up)[step // local][index : index + 1, :] = value

        @pl.loop(1, members)
        def _(j):
            scale_copy(step, j).start()

    def scale_and_send(step, slot, reload):
        @pl.loop(1, members)
        def _(j):
            scale_copy(step, j).wait_recv()

        if step >= RING:
            own_copy(step - RING).wait()

            @pl.loop(1, members)
            def _(j):
                data_copy(step - RING, j).wait_send()

        @pl.loop(0, members)
        def _(j):
            if reload:
                load(step, slot, j).wait()
            inverse = 1.0 / scales[step, lax.rem(members - j, members)]
            narrow[step % RING, j] = (held[slot, j] * inverse).astype(jnp.bfloat16)

        @pl.loop(1, members)
        def _(j):
            data_copy(step, j).start()

        own_copy(step).start()

    sums(0, 0)
    ready = 0
    for step in range(1, steps):
        place = step - 1
        sums(step, 1 + place % RING)
        start_place(place + RING)
        if step >= RING:
            total(ready)
            ready += 1
    if ready == 0:
        total(0)
        ready = 1
    scale_and_send(0, 0, False)
    for step in range(ready, steps):
        total(step)

    router_own = pltpu.make_async_copy(part_router, my_block, router_sem.at[0])
    router_own.start()
    for j in range(1, members):
        row_copy(j).start()

    for step in range(1, steps):
        place = steps - 2 + step
        scale_and_send(step, 1 + place % RING, True)
        start_place(place + RING)

    router_own.wait()
    for j in range(1, members):
        row_copy(j).wait()
    for j in range(1, groups):
        col_copy(j).start()

    for step in range(steps):
        @pl.loop(1, members)
        def _(j):
            sum_copy(step, j).wait_send()
            scale_copy(step, j).wait_send()
            data_copy(step, j).wait_recv()

        if step >= steps - RING:
            own_copy(step).wait()

            @pl.loop(1, members)
            def _(j):
                data_copy(step, j).wait_send()

    for j in range(1, groups):
        col_copy(j).wait()


def exchange(groups, members, master_gate, master_up, part_router):
    experts, rows, inner = master_gate.shape
    local = experts // members
    steps = 2 * local
    width, depth = part_router.shape
    anywhere = pl.BlockSpec(memory_space=pl.ANY)
    in_vmem = pl.BlockSpec(memory_space=pltpu.VMEM)
    final = jax.ShapeDtypeStruct((local, members * rows, inner), jnp.bfloat16)
    scale = jax.ShapeDtypeStruct((local, inner), jnp.float32)
    dma = pltpu.SemaphoreType.DMA
    return pl.pallas_call(
        functools.partial(kernel, groups, members, local, rows),
        out_shape=(
            final, final, scale, scale,
            jax.ShapeDtypeStruct((groups * width, members * depth), jnp.bfloat16),
        ),
        in_specs=[anywhere] * 3,
        out_specs=(anywhere, anywhere, in_vmem, in_vmem, anywhere),
        scratch_shapes=[
            pltpu.VMEM((1 + RING, members, rows, inner), jnp.float32),
            pltpu.VMEM((RING, members, rows, inner), jnp.bfloat16),
            pltpu.VMEM((steps, members, 1, inner), jnp.float32),
            pltpu.VMEM((steps, members, 1, inner), jnp.float32),
            pltpu.VMEM((steps, members, 1, inner), jnp.float32),
            dma((1 + RING, members)),
            dma((steps, members)), dma((steps, members)), dma((steps,)),
            dma((steps, members)), dma((steps, members)),
            dma((steps, members)), dma((steps, members)),
            dma((members,)), dma((members,)), dma((groups,)), dma((groups,)), dma((1,)),
        ],
        compiler_params=pltpu.CompilerParams(
            collective_id=0, has_side_effects=True, vmem_limit_bytes=56 * 1024 * 1024
        ),
    )(master_gate, master_up, part_router)


def solution(mesh):
    groups, members = mesh.shape["ep"], mesh.shape["fsdp"]

    def body(master_gate, master_up, router_weight, router_gain):
        part_router = (router_weight * router_gain[:, None]).astype(jnp.bfloat16).T
        final_gate, final_up, scale_gate, scale_up, router = exchange(
            groups, members, master_gate, master_up, part_router
        )
        return (final_gate, final_up, scale_gate, scale_up, router.T)

    return jax.shard_map(
        body,
        mesh=mesh,
        in_specs=(P("ep", "fsdp", None), P("ep", "fsdp", None), P("fsdp", "ep"), P("fsdp")),
        out_specs=(
            P(("ep", "fsdp"), None, None),
            P(("ep", "fsdp"), None, None),
            P(("ep", "fsdp"), None),
            P(("ep", "fsdp"), None),
            P(),
        ),
        check_vma=False,
    )
```

```python
import functools

import jax
import jax.numpy as jnp
from jax import lax
from jax.experimental import pallas as pl
from jax.experimental.pallas import tpu as pltpu
from jax.sharding import PartitionSpec as P

MESH = pl.DeviceIdType.MESH
RING = 2
SLOTS = 3


def kernel(
    groups, members, local, rows,
    gate, up, part_router,
    final_gate, final_up, scale_gate, scale_up, router,
    held, narrow, partial, arrived, scales,
    load_sem, send_sem, recv_sem,
    sum_send, sum_recv, scale_send, scale_recv,
    row_send, row_recv, col_send, col_recv, router_sem,
):
    group, me = lax.axis_index("ep"), lax.axis_index("fsdp")
    steps = 2 * local

    def peer(j):
        return lax.rem(me + j, members)

    def group_peer(j):
        return lax.rem(group + j, groups)

    def source(step):
        return (gate, up)[step // local], (final_gate, final_up)[step // local], step % local

    order = [*range(1, steps), *range(1, steps)]

    def load(step, slot, j):
        master, _, index = source(step)
        return pltpu.make_async_copy(
            master.at[peer(j) * local + index], held.at[slot, j], load_sem.at[slot, j]
        )

    def start_load(step, slot):
        @pl.loop(0, members)
        def _(j):
            load(step, slot, j).start()

    def start_place(place):
        if place < len(order):
            start_load(order[place], 1 + place % RING)

    def sum_copy(step, j):
        return pltpu.make_async_remote_copy(
            src_ref=partial.at[step, j], dst_ref=arrived.at[step, j],
            send_sem=sum_send.at[step, j], recv_sem=sum_recv.at[step, j],
            device_id=(group, peer(j)), device_id_type=MESH,
        )

    def scale_copy(step, j):
        return pltpu.make_async_remote_copy(
            src_ref=scales.at[step, 0], dst_ref=scales.at[step, j],
            send_sem=scale_send.at[step, j], recv_sem=scale_recv.at[step, j],
            device_id=(group, peer(j)), device_id_type=MESH,
        )

    def my_rows(final, index):
        return final.at[index, pl.ds(pl.multiple_of(me * rows, rows), rows), :]

    def data_copy(step, j):
        _, final, index = source(step)
        return pltpu.make_async_remote_copy(
            src_ref=narrow.at[step % SLOTS, j], dst_ref=my_rows(final, index),
            send_sem=send_sem.at[step, j], recv_sem=recv_sem.at[step, j],
            device_id=(group, peer(j)), device_id_type=MESH,
        )

    width, depth = part_router.shape
    my_group_rows = pl.ds(pl.multiple_of(group * width, width), width)
    my_block = router.at[my_group_rows, pl.ds(pl.multiple_of(me * depth, depth), depth)]

    def row_copy(j):
        return pltpu.make_async_remote_copy(
            src_ref=part_router, dst_ref=my_block, send_sem=row_send.at[j], recv_sem=row_recv.at[j],
            device_id=(group, near_peer(j)), device_id_type=MESH,
        )

    half = members // 2
    near = [*range(1, half), half]

    def near_peer(j):
        if j == half:
            return peer(half)
        return me // half * half + lax.rem(me % half + j, half)

    def relay_copy(j):
        other = pl.ds(pl.multiple_of(peer(half) * depth, depth), depth)
        block = router.at[my_group_rows, other]
        return pltpu.make_async_remote_copy(
            src_ref=block, dst_ref=block, send_sem=row_send.at[half + j], recv_sem=row_recv.at[half + j],
            device_id=(group, near_peer(j)), device_id_type=MESH,
        )

    def col_copy(j):
        return pltpu.make_async_remote_copy(
            src_ref=router.at[my_group_rows, :], dst_ref=router.at[my_group_rows, :],
            send_sem=col_send.at[j], recv_sem=col_recv.at[j],
            device_id=(group_peer(j), me), device_id_type=MESH,
        )

    start_load(0, 0)
    for place in range(RING):
        start_place(place)

    barrier = pltpu.get_barrier_semaphore()
    for j in range(1, members):
        pl.semaphore_signal(barrier, inc=1, device_id=(group, peer(j)), device_id_type=MESH)
    for j in range(1, groups):
        pl.semaphore_signal(barrier, inc=1, device_id=(group_peer(j), me), device_id_type=MESH)
    pl.semaphore_wait(barrier, members + groups - 2)

    def sums(step, slot):
        @pl.loop(0, members)
        def _(j):
            load(step, slot, j).wait()
            block = held[slot, j]
            partial[step, j] = jnp.sum(block * block, axis=0, keepdims=True)

        @pl.loop(1, members)
        def _(j):
            sum_copy(step, j).start()

    def total(step):
        @pl.loop(1, members)
        def _(j):
            sum_copy(step, j).wait_recv()

        value = partial[step, 0]
        for j in range(1, members):
            value = value + arrived[step, j]
        value = jnp.sqrt(value)
        scales[step, 0] = value
        index = step % local
        (scale_gate, scale_up)[step // local][index : index + 1, :] = value

        @pl.loop(1, members)
        def _(j):
            scale_copy(step, j).start()

    def scale_and_send(step, slot, reload):
        @pl.loop(1, members)
        def _(j):
            scale_copy(step, j).wait_recv()

        if step >= SLOTS:
            @pl.loop(1, members)
            def _(j):
                data_copy(step - SLOTS, j).wait_send()

        @pl.loop(1, members)
        def _(j):
            if reload:
                load(step, slot, j).wait()
            inverse = 1.0 / scales[step, lax.rem(members - j, members)]
            narrow[step % SLOTS, j] = (held[slot, j] * inverse).astype(jnp.bfloat16)

        @pl.loop(1, members)
        def _(j):
            data_copy(step, j).start()

        if reload:
            load(step, slot, 0).wait()
        _, final, index = source(step)
        own = held[slot, 0] * (1.0 / scales[step, 0])
        final[index, pl.ds(pl.multiple_of(me * rows, rows), rows), :] = own.astype(jnp.bfloat16)

    sums(0, 0)
    lead = min(SLOTS, steps)
    for step in range(1, lead):
        sums(step, 1 + (step - 1) % RING)
        start_place(step - 1 + RING)
    total(0)
    scale_and_send(0, 0, False)
    for step in range(lead, steps):
        sums(step, 1 + (step - 1) % RING)
        start_place(step - 1 + RING)
    for step in range(1, lead):
        total(step)

    router_own = pltpu.make_async_copy(part_router, my_block, router_sem.at[0])
    router_own.start()
    for j in near:
        row_copy(j).start()

    for step in range(1, steps):
        if step == 2:
            for late in range(lead, steps):
                total(late)
        place = steps - 2 + step
        scale_and_send(step, 1 + place % RING, True)
        start_place(place + RING)
        if step == steps // 2:
            for j in near:
                row_copy(j).wait()
            for j in range(1, members // 2):
                relay_copy(j).start()

    router_own.wait()
    for j in range(1, members // 2):
        relay_copy(j).wait()
    for j in range(1, groups):
        col_copy(j).start()

    for step in range(steps):
        @pl.loop(1, members)
        def _(j):
            sum_copy(step, j).wait_send()
            scale_copy(step, j).wait_send()
            data_copy(step, j).wait_recv()

        if step >= steps - SLOTS:
            @pl.loop(1, members)
            def _(j):
                data_copy(step, j).wait_send()

    for j in range(1, groups):
        col_copy(j).wait()


def exchange(groups, members, master_gate, master_up, part_router):
    experts, rows, inner = master_gate.shape
    local = experts // members
    steps = 2 * local
    width, depth = part_router.shape
    anywhere = pl.BlockSpec(memory_space=pl.ANY)
    in_vmem = pl.BlockSpec(memory_space=pltpu.VMEM)
    final = pltpu.VMEM((local, members * rows, inner), jnp.bfloat16)
    scale = jax.ShapeDtypeStruct((local, inner), jnp.float32)
    dma = pltpu.SemaphoreType.DMA
    return pl.pallas_call(
        functools.partial(kernel, groups, members, local, rows),
        out_shape=(
            final, final, scale, scale,
            jax.ShapeDtypeStruct((groups * width, members * depth), jnp.bfloat16),
        ),
        in_specs=[anywhere] * 3,
        out_specs=(in_vmem, in_vmem, in_vmem, in_vmem, anywhere),
        scratch_shapes=[
            pltpu.VMEM((1 + RING, members, rows, inner), jnp.float32),
            pltpu.VMEM((SLOTS, members, rows, inner), jnp.bfloat16),
            pltpu.VMEM((steps, members, 1, inner), jnp.float32),
            pltpu.VMEM((steps, members, 1, inner), jnp.float32),
            pltpu.VMEM((steps, members, 1, inner), jnp.float32),
            dma((1 + RING, members)),
            dma((steps, members)), dma((steps, members)),
            dma((steps, members)), dma((steps, members)),
            dma((steps, members)), dma((steps, members)),
            dma((members,)), dma((members,)), dma((groups,)), dma((groups,)), dma((1,)),
        ],
        compiler_params=pltpu.CompilerParams(
            collective_id=0, has_side_effects=True, vmem_limit_bytes=34 * 1024 * 1024
        ),
    )(master_gate, master_up, part_router)


def store_kernel(gate, up, final_gate, final_up, sem):
    copies = [
        pltpu.make_async_copy(landed.at[index], final.at[index], sem.at[which, index])
        for which, (landed, final) in enumerate(((gate, final_gate), (up, final_up)))
        for index in range(landed.shape[0])
    ]
    for copy in copies:
        copy.start()
    for copy in copies:
        copy.wait()


def store(gate, up):
    final = jax.ShapeDtypeStruct(gate.shape, gate.dtype)
    return pl.pallas_call(
        store_kernel,
        out_shape=(final, final),
        in_specs=[pl.BlockSpec(memory_space=pltpu.VMEM)] * 2,
        out_specs=(pl.BlockSpec(memory_space=pl.ANY),) * 2,
        scratch_shapes=[pltpu.SemaphoreType.DMA((2, gate.shape[0]))],
        compiler_params=pltpu.CompilerParams(vmem_limit_bytes=2 * 1024 * 1024),
    )(gate, up)


def solution(mesh):
    groups, members = mesh.shape["ep"], mesh.shape["fsdp"]

    def body(master_gate, master_up, router_weight, router_gain):
        part_router = (router_weight * router_gain[:, None]).astype(jnp.bfloat16).T
        final_gate, final_up, scale_gate, scale_up, router = exchange(
            groups, members, master_gate, master_up, part_router
        )
        final_gate, final_up = store(final_gate, final_up)
        return (final_gate, final_up, scale_gate, scale_up, router.T)

    return jax.shard_map(
        body,
        mesh=mesh,
        in_specs=(P("ep", "fsdp", None), P("ep", "fsdp", None), P("fsdp", "ep"), P("fsdp")),
        out_specs=(
            P(("ep", "fsdp"), None, None),
            P(("ep", "fsdp"), None, None),
            P(("ep", "fsdp"), None),
            P(("ep", "fsdp"), None),
            P(),
        ),
        check_vma=False,
    )
```
